32 devices in a mesh: qa: 16 (over z, x, core), qb: 2 (over y).
Axes of the slice: x: 2, y: 2, z: 4, core: 2. Of those that a mesh axis runs over, the one named last changes fastest.
Arguments:
- wave_parts: float32 [2, 256, 128, 128], P(None, ('qa', 'qb')), may hold values from -6 to 6
- level_table: float32 [256, 128, 128], P(('qa', 'qb')), may hold values from -2 to 2
- phase_angles: float32 [2, 128], replicated, may hold values from 0.3 to 1.2
Outputs:
- final_parts: float32 [2, 256, 128, 128], P(None, ('qa', 'qb'))
The draws below stay inside these ranges and needn't reach their ends.
All inputs are finite; a program needn't handle non-finite values.
Results may differ from the reference program's by a relative error of at most 0.0003.
Values sent between devices are 32-bit elements; how exact they have to be, the bound alone decides.
A program may use at most 64 MiB of HBM per device.

```python
import jax
import jax.numpy as jnp
from jax import lax

BLOCKS_DEV = 8
ROWS = 128
LANES = 128
BLOCKS = 256
LAYERS = 2
N_QA = 16
N_QB = 2


def shard_levels(stream_key, dims, cuts, low, top_value):
    def one(position, blocks):
        heights = jax.random.uniform(jax.random.fold_in(jax.random.fold_in(stream_key, 6), position), (blocks,), jnp.float32, low / len(cuts), top_value / len(cuts))
        return jnp.repeat(jnp.exp(heights), dims[position] // blocks).reshape((-1,) + (1,) * (len(dims) - position - 1))

    gain = one(*cuts[0])
    for cut in cuts[1:]:
        gain = gain * one(*cut)
    return gain


def bell_draw(key, dims, width, most, pieces=(), kind=jnp.bfloat16):
    level = shard_levels(key, dims, pieces, -0.22, 0.18) if pieces else 1.0
    result = jax.random.normal(key, dims, jnp.float32) * width * level
    return jnp.minimum(jnp.maximum(result, -most), most).astype(kind)


def setup_inputs(seed: int = 0) -> dict:
    seeds = jax.random.split(jax.random.key(seed), 4)
    wave_parts = bell_draw(seeds[0], (2, BLOCKS, ROWS, LANES), 1.0, 6.0, ((1, 32),), jnp.float32)
    level_table = jnp.clip(jax.random.uniform(seeds[1], (BLOCKS, ROWS, LANES), jnp.float32, -2.0, 2.0) * shard_levels(seeds[1], (BLOCKS, ROWS, LANES), ((0, 32),), -0.4, 0.0), -2.0, 2.0)
    phase_angles = jnp.clip(jax.random.uniform(seeds[2], (LAYERS, LANES), jnp.float32, 0.3, 1.2), 0.3, 1.2)
    return {"wave_parts": wave_parts, "level_table": level_table, "phase_angles": phase_angles}


def count_bits(values, count):
    places = jnp.arange(count.bit_length() - 1, dtype=jnp.int32)
    return jnp.sum((values[..., None] >> places) & 1, axis=-1)


def sign_table(count):
    rank = jnp.arange(count, dtype=jnp.int32)
    parity = count_bits(rank[:, None] & rank[None, :], count) % 2
    real_part = jnp.where(parity == 1, -1.0, 1.0).astype(jnp.float32) * (count ** -0.5)
    return real_part


def turn_dim(values, dim):
    real_part = sign_table(values.shape[dim])
    def times(table):
        moved = jnp.tensordot(values, table, axes=([dim], [0]), precision=lax.Precision.HIGHEST)
        return jnp.moveaxis(moved, -1, dim)
    return times(real_part)


def turn_phase(values, levels, angle):
    turn = angle * levels
    return jnp.stack([values[0] * jnp.cos(turn) + values[1] * jnp.sin(turn), values[1] * jnp.cos(turn) - values[0] * jnp.sin(turn)])


def reference(wave_parts, level_table, phase_angles):
    values = wave_parts
    for layer in range(LAYERS):
        values = turn_phase(values, level_table, phase_angles[layer])
        values = turn_dim(values, 3)
        values = turn_dim(values, 2)
        parts = values.reshape(2, N_QA, N_QB, BLOCKS_DEV, ROWS, LANES)
        parts = turn_dim(parts, 1)
        parts = turn_dim(parts, 2)
        parts = turn_dim(parts, 3)
        values = parts.reshape(values.shape)
    return values
```

```python
import functools

import jax
import jax.numpy as jnp
import numpy as np
from jax import lax
from jax.experimental import pallas as pl
from jax.experimental.pallas import tpu as pltpu
from jax.sharding import PartitionSpec as P

MESH = pl.DeviceIdType.MESH
TURN_MOST = 2.5


def fit_even(function, degree):
    top = TURN_MOST**2
    nodes = (np.cos(np.pi * (np.arange(64) + 0.5) / 64) + 1) * top / 2
    fit = np.polynomial.chebyshev.Chebyshev.fit(nodes, function(np.sqrt(nodes)), degree, domain=[0, top])
    return [float(c) for c in fit.convert(kind=np.polynomial.Polynomial).coef]


COS = fit_even(np.cos, 6)
SIN = fit_even(lambda t: np.sin(t) / t, 5)


def horner(coefs, u):
    total = jnp.float32(coefs[-1])
    for c in coefs[-2::-1]:
        total = total * u + jnp.float32(c)
    return total


def cos_sin(turn):
    u = turn * turn
    return horner(COS, u), turn * horner(SIN, u)


def sign_table(count, power):
    rank = np.arange(count)
    parity = np.zeros((count, count), np.int64)
    both = rank[:, None] & rank[None, :]
    while both.any():
        parity ^= both & 1
        both >>= 1
    return jnp.asarray((1.0 - 2.0 * parity) * 2.0**-power, jnp.bfloat16)


def mix_lead(x):
    n = x.shape[0]
    half = 1
    while half < n:
        y = x.reshape((n // (2 * half), 2, half) + x.shape[1:])
        x = jnp.stack([y[:, 0] + y[:, 1], y[:, 0] - y[:, 1]], axis=1).reshape(x.shape)
        half *= 2
    return x


def halves(x):
    hi = x.astype(jnp.bfloat16)
    return hi, (x - hi.astype(jnp.float32)).astype(jnp.bfloat16)


def mix_rows(table, x):
    hi, lo = halves(x)
    return jnp.dot(table, hi, preferred_element_type=jnp.float32) + jnp.dot(table, lo, preferred_element_type=jnp.float32)


def mix_lanes(x, table):
    hi, lo = halves(x)
    return jnp.dot(hi, table, preferred_element_type=jnp.float32) + jnp.dot(lo, table, preferred_element_type=jnp.float32)


def kernel(
    na, nb, wave_hbm, level_hbm, angle_ref, row0, lane0, row1, lane1, out_ref,
    wave, level, send0, got0, send1, got1, levels, cosine, sine,
    load_sem, own_sem, ssem, rsem,
):
    n = na * nb
    _, blocks, rows, lanes = wave.shape
    piece = send0.shape[2]
    per = rows // piece
    qa, qb = lax.axis_index("qa"), lax.axis_index("qb")
    me = qa * nb + qb

    def peer(k):
        to_a = lax.rem(qa + k // nb, na)
        to_b = lax.rem(qb + lax.rem(k, nb), nb)
        return to_a, to_b, to_a * nb + to_b

    barrier = pltpu.get_barrier_semaphore()

    @pl.loop(1, n)
    def _(k):
        to_a, to_b, _ = peer(k)
        pl.semaphore_signal(barrier, inc=1, device_id=(to_a, to_b), device_id_type=MESH)

    load_wave = pltpu.make_async_copy(wave_hbm, wave, load_sem.at[0])
    load_level = pltpu.make_async_copy(level_hbm, level, load_sem.at[1])
    load_level.start()
    load_wave.start()
    pl.semaphore_wait(barrier, n - 1)

    def exchange(source, target, slot):
        own = pltpu.make_async_copy(source.at[me], target.at[me], own_sem.at[slot])
        own.start()

        @pl.loop(0, n - 1)
        def _(i):
            k = lax.rem(i + (n // 2), n - 1) + 1
            to_a, to_b, to = peer(k)
            pltpu.make_async_remote_copy(
                src_ref=source.at[to], dst_ref=target.at[me], send_sem=ssem.at[slot], recv_sem=rsem.at[slot],
                device_id=(to_a, to_b), device_id_type=MESH,
            ).start()

        return own

    def finish(own, source, target, slot, sent):
        if not sent:
            own.wait()
        rest = (source if sent else target).at[pl.ds(0, n - 1)]
        pltpu.make_async_copy(rest, rest, (ssem if sent else rsem).at[slot]).wait()

    load_level.wait()
    own_levels = exchange(level, levels, 0)
    load_wave.wait()

    first = angle_ref[0:1, :]

    @pl.loop(0, blocks)
    def _(b):
        held = level[pl.ds(b * per, per)].reshape(rows, lanes)
        c, s = cos_sin(first * held)
        x, y = wave[0, b], wave[1, b]
        both = jnp.concatenate([x * c + y * s, y * c - x * s], axis=1)
        both = mix_rows(row0[...], both)
        wave[0, b] = mix_lanes(both[:, :lanes], lane0[...])
        wave[1, b] = mix_lanes(both[:, lanes:], lane0[...])

    for part in range(2):

        @pl.loop(0, rows // 16)
        def _(j):
            mixed = mix_lead(wave[part, :, pl.ds(pl.multiple_of(j * 16, 16), 16), :])
            for b in range(blocks):
                scatter(send0, part, b, j, mixed[b], per, piece)

    own0 = exchange(send0, got0, 1)

    finish(own_levels, level, levels, 0, False)
    second = angle_ref[1:2, :]

    @pl.loop(0, n)
    def _(d):
        c, s = cos_sin(second * levels[d])
        cosine[d] = c
        sine[d] = s

    finish(own0, send0, got0, 1, False)
    step = min(8, piece)

    @pl.loop(0, piece // step)
    def _(j):
        part = pl.ds(pl.multiple_of(j * step, step), step)
        x, y = mix_lead(got0[:, 0, part, :]), mix_lead(got0[:, 1, part, :])
        c, s = cosine[:, part, :], sine[:, part, :]
        send1[:, 0, part, :] = mix_lead(x * c + y * s)
        send1[:, 1, part, :] = mix_lead(y * c - x * s)

    own1 = exchange(send1, got1, 2)
    finish(own_levels, levels, levels, 0, True)
    finish(own0, send0, got0, 1, True)
    finish(own1, send1, got1, 2, False)

    @pl.loop(0, blocks)
    def _(b):
        held = pl.ds(b * per, per)
        both = jnp.concatenate(
            [got1[held, 0].reshape(rows, lanes), got1[held, 1].reshape(rows, lanes)], axis=1
        )
        both = mix_rows(row1[...], both)
        wave[0, b] = mix_lanes(both[:, :lanes], lane1[...])
        wave[1, b] = mix_lanes(both[:, lanes:], lane1[...])

    for part in range(2):

        @pl.loop(0, rows // 16)
        def _(j):
            held = pl.ds(pl.multiple_of(j * 16, 16), 16)
            out_ref[part, :, held, :] = mix_lead(wave[part, :, held, :])

    finish(own1, send1, got1, 2, True)


def scatter(send, part, b, j, values, per, piece):
    if piece >= 16:
        steps = piece // 16
        send[b * per + j // steps, part, pl.ds(pl.multiple_of(lax.rem(j, steps) * 16, 16), 16), :] = values
    else:
        for i in range(16 // piece):
            send[b * per + j * (16 // piece) + i, part] = values[i * piece : (i + 1) * piece]


def body(wave_parts, level_table, phase_angles):
    na, nb = lax.axis_size("qa"), lax.axis_size("qb")
    n = na * nb
    _, blocks, rows, lanes = wave_parts.shape
    piece = blocks * rows // n
    bits = (n * blocks * rows * lanes).bit_length() - 1
    powers = [(bits + i) // 4 for i in range(4)]
    tables = [sign_table(rows if i % 2 == 0 else lanes, p) for i, p in enumerate(powers)]
    vmem = pl.BlockSpec(memory_space=pltpu.VMEM)
    hbm = pl.BlockSpec(memory_space=pl.ANY)
    f32 = jnp.float32
    state = pltpu.VMEM((n, 2, piece, lanes), f32)
    table = pltpu.VMEM((n, piece, lanes), f32)
    return pl.pallas_call(
        functools.partial(kernel, na, nb),
        out_shape=jax.ShapeDtypeStruct(wave_parts.shape, f32),
        in_specs=[hbm, hbm, vmem, vmem, vmem, vmem, vmem],
        out_specs=vmem,
        scratch_shapes=[
            pltpu.VMEM(wave_parts.shape, f32),
            table,
            state, state, state, state, table, table, table,
            pltpu.SemaphoreType.DMA((2,)),
            pltpu.SemaphoreType.DMA((3,)),
            pltpu.SemaphoreType.DMA((3,)),
            pltpu.SemaphoreType.DMA((3,)),
        ],
        compiler_params=pltpu.CompilerParams(
            collective_id=0, has_side_effects=True, vmem_limit_bytes=40 * 2**20
        ),
    )(wave_parts, level_table.reshape(n, piece, lanes), phase_angles, *tables)


def solution(mesh):
    in_specs = (P(None, ("qa", "qb"), None, None), P(("qa", "qb"), None, None), P())
    out_specs = P(None, ("qa", "qb"), None, None)
    return jax.shard_map(body, mesh=mesh, in_specs=in_specs, out_specs=out_specs, check_vma=False)
```

```python
import functools

import jax
import jax.numpy as jnp
import numpy as np
from jax import lax
from jax.experimental import pallas as pl
from jax.experimental.pallas import tpu as pltpu
from jax.sharding import PartitionSpec as P

MESH = pl.DeviceIdType.MESH
TURN_MOST = 2.5


def fit_even(function, degree):
    top = TURN_MOST**2
    nodes = (np.cos(np.pi * (np.arange(64) + 0.5) / 64) + 1) * top / 2
    fit = np.polynomial.chebyshev.Chebyshev.fit(nodes, function(np.sqrt(nodes)), degree, domain=[0, top])
    return [float(c) for c in fit.convert(kind=np.polynomial.Polynomial).coef]


COS = fit_even(np.cos, 6)
SIN = fit_even(lambda t: np.sin(t) / t, 5)


def horner(coefs, u, scale):
    total = jnp.float32(coefs[-1] * scale)
    for c in coefs[-2::-1]:
        total = total * u + jnp.float32(c * scale)
    return total


def cos_sin(turn, scale):
    u = turn * turn
    return horner(COS, u, scale), turn * horner(SIN, u, scale)


def sign_table(count):
    both = lax.broadcasted_iota(jnp.int32, (count, count), 0) & lax.broadcasted_iota(jnp.int32, (count, count), 1)
    shift = 1
    while shift < count.bit_length():
        shift *= 2
    while shift > 1:
        shift //= 2
        both = both ^ (both >> shift)
    return (1 - 2 * (both & 1)).astype(jnp.float32).astype(jnp.bfloat16)


def mix_lead(x):
    n = x.shape[0]
    half = 1
    while half < n:
        y = x.reshape((n // (2 * half), 2, half) + x.shape[1:])
        x = jnp.stack([y[:, 0] + y[:, 1], y[:, 0] - y[:, 1]], axis=1).reshape(x.shape)
        half *= 2
    return x


def dot(a, b):
    return jnp.dot(a, b, preferred_element_type=jnp.float32)


def halves(x):
    hi = x.astype(jnp.bfloat16)
    return hi, (x - hi.astype(jnp.float32)).astype(jnp.bfloat16)


def mix_rows_lanes(rows, lanes, x, y):
    hi, lo = halves(jnp.concatenate([x, y], axis=1))
    both = dot(rows, hi) + dot(rows, lo)
    width = x.shape[1]
    out = []
    for part in (both[:, :width], both[:, width:]):
        hi, lo = halves(part)
        out.append(dot(hi, lanes) + dot(lo, lanes))
    return out


def kernel(
    na, nb, scales, wave_hbm, level_hbm, angle_hbm, out_ref,
    wave, level, angle, rows_table, lanes_table, mixed, send0, got0, send1, got1, levels, cosine, sine,
    load_sem, own_sem, ssem, rsem, level_sem,
):
    n = na * nb
    cuts, _, _, step, lanes = send0.shape
    qa, qb = lax.axis_index("qa"), lax.axis_index("qb")
    me = qa * nb + qb

    def flips(q, count):
        found = [q]
        bit = 1
        while bit < count:
            change = bit - 2 * bit * lax.rem(q // bit, 2)
            found = found + [f + change for f in found]
            bit *= 2
        return found

    to_as, to_bs = flips(qa, na), flips(qb, nb)
    order = [(ka, kb) for ka in far_first(na) for kb in range(nb - 1, -1, -1) if ka or kb]
    peers = [(to_as[ka], to_bs[kb], to_as[ka] * nb + to_bs[kb]) for ka, kb in order]

    load_wave = pltpu.make_async_copy(wave_hbm, wave, load_sem.at[0])
    load_level = pltpu.make_async_copy(level_hbm, level, load_sem.at[1])
    load_angle = pltpu.make_async_copy(angle_hbm, angle, load_sem.at[2])
    load_level.start()
    load_angle.start()
    load_wave.start()

    barrier = pltpu.get_barrier_semaphore()
    for to_a, to_b, _ in peers:
        pl.semaphore_signal(barrier, inc=1, device_id=(to_a, to_b), device_id_type=MESH)

    rows_table[...] = sign_table(n * step)
    lanes_table[...] = sign_table(lanes)
    load_level.wait()
    pl.semaphore_wait(barrier, n - 1)

    def exchange(source, target, own, sent, got):
        pltpu.make_async_copy(source.at[me], target.at[me], own).start()
        for to_a, to_b, to in peers:
            pltpu.make_async_remote_copy(
                src_ref=source.at[to], dst_ref=target.at[me], send_sem=sent, recv_sem=got,
                device_id=(to_a, to_b), device_id_type=MESH,
            ).start()

    def received(source, target, own, got):
        pltpu.make_async_copy(source.at[me], target.at[me], own).wait()
        rest = target.at[pl.ds(0, n - 1)]
        pltpu.make_async_copy(rest, rest, got).wait()

    def left(source, sent):
        rest = source.at[pl.ds(0, n - 1)]
        pltpu.make_async_copy(rest, rest, sent).wait()

    exchange(level, levels, level_sem.at[0], level_sem.at[1], level_sem.at[2])
    load_angle.wait()
    load_wave.wait()

    first = angle[0:1, :]

    @pl.loop(0, cuts)
    def _(cut):
        held = pl.ds(pl.multiple_of(cut * step, step), step)
        c, s = cos_sin(first * level[:, held, :].reshape(n * step, lanes), scales[0])
        x = wave[0, :, held, :].reshape(n * step, lanes)
        y = wave[1, :, held, :].reshape(n * step, lanes)
        done = mix_rows_lanes(rows_table[...], lanes_table[...], x * c + y * s, y * c - x * s)
        for part in range(2):
            mixed[cut, part] = done[part].reshape(n, step, lanes)

    group = 4
    for part in range(2):

        @pl.loop(0, n // group)
        def _(i):
            ds = pl.ds(i * group, group)
            send0[:, ds, part] = mix_lead(mixed[:, part, ds])

    @pl.loop(0, cuts)
    def _(cut):
        exchange(send0.at[cut], got0.at[cut], own_sem.at[0, cut], ssem.at[0, cut], rsem.at[0, cut])

    received(level, levels, level_sem.at[0], level_sem.at[2])
    second = angle[1:2, :]

    @pl.loop(0, n)
    def _(d):
        c, s = cos_sin(second * levels[d], scales[1])
        cosine[d] = c
        sine[d] = s

    @pl.loop(0, cuts)
    def _(cut):
        received(send0.at[cut], got0.at[cut], own_sem.at[0, cut], rsem.at[0, cut])
        held = pl.ds(pl.multiple_of(cut * step, step), step)
        x, y = mix_lead(got0[cut, :, 0]), mix_lead(got0[cut, :, 1])
        c, s = cosine[:, held, :], sine[:, held, :]
        send1[cut, :, 0] = mix_lead(x * c + y * s)
        send1[cut, :, 1] = mix_lead(y * c - x * s)
        exchange(send1.at[cut], got1.at[cut], own_sem.at[1, cut], ssem.at[1, cut], rsem.at[1, cut])

    @pl.loop(0, cuts)
    def _(cut):
        received(send1.at[cut], got1.at[cut], own_sem.at[1, cut], rsem.at[1, cut])
        x, y = (got1[cut, :, part].reshape(n * step, lanes) for part in range(2))
        done = mix_rows_lanes(rows_table[...], lanes_table[...], x, y)
        for part in range(2):
            mixed[cut, part] = done[part].reshape(n, step, lanes)

    for part in range(2):

        @pl.loop(0, n // group)
        def _(i):
            ds = pl.ds(i * group, group)
            done = mix_lead(mixed[:, part, ds])
            for cut in range(cuts):
                out_ref[part, ds, cut * step : (cut + 1) * step, :] = done[cut]

    left(level, level_sem.at[1])

    @pl.loop(0, cuts)
    def _(cut):
        left(send0.at[cut], ssem.at[0, cut])
        left(send1.at[cut], ssem.at[1, cut])


def far_first(count):
    return range(count - 1, -1, -1)


STEP = 8


def body(wave_parts, level_table, phase_angles):
    na, nb = lax.axis_size("qa"), lax.axis_size("qb")
    n = na * nb
    _, blocks, rows, lanes = wave_parts.shape
    piece = blocks * rows // n
    step = min(STEP, piece)
    cuts = piece // step
    bits = (n * blocks * rows * lanes).bit_length() - 1
    scales = (2.0 ** -(bits // 2), 2.0 ** -(bits - bits // 2))
    hbm = pl.BlockSpec(memory_space=pl.ANY)
    f32 = jnp.float32
    flat = (2, n, piece, lanes)
    state = pltpu.VMEM((cuts, n, 2, step, lanes), f32)
    table = pltpu.VMEM((n, piece, lanes), f32)
    result = pl.pallas_call(
        functools.partial(kernel, na, nb, scales),
        out_shape=jax.ShapeDtypeStruct(flat, f32),
        in_specs=[hbm, hbm, hbm],
        out_specs=pl.BlockSpec(memory_space=pltpu.VMEM),
        scratch_shapes=[
            pltpu.VMEM(flat, f32),
            table,
            pltpu.VMEM(phase_angles.shape, f32),
            pltpu.VMEM((n * step, n * step), jnp.bfloat16),
            pltpu.VMEM((lanes, lanes), jnp.bfloat16),
            pltpu.VMEM((cuts, 2, n, step, lanes), f32),
            state, state, state, state, table, table, table,
            pltpu.SemaphoreType.DMA((3,)),
            pltpu.SemaphoreType.DMA((2, cuts)),
            pltpu.SemaphoreType.DMA((2, cuts)),
            pltpu.SemaphoreType.DMA((2, cuts)),
            pltpu.SemaphoreType.DMA((3,)),
        ],
        compiler_params=pltpu.CompilerParams(
            collective_id=0, has_side_effects=True, vmem_limit_bytes=50 * 2**20
        ),
    )(wave_parts.reshape(flat), level_table.reshape(n, piece, lanes), phase_angles)
    return result.reshape(wave_parts.shape)


def solution(mesh):
    in_specs = (P(None, ("qa", "qb"), None, None), P(("qa", "qb"), None, None), P())
    out_specs = P(None, ("qa", "qb"), None, None)
    return jax.shard_map(body, mesh=mesh, in_specs=in_specs, out_specs=out_specs, check_vma=False)
```

```python
import functools

import jax
import jax.numpy as jnp
import numpy as np
from jax import lax
from jax.experimental import pallas as pl
from jax.experimental.pallas import tpu as pltpu
from jax.sharding import PartitionSpec as P

MESH = pl.DeviceIdType.MESH
TURN_MOST = 2.5


def fit_even(function, degree):
    top = TURN_MOST**2
    nodes = (np.cos(np.pi * (np.arange(64) + 0.5) / 64) + 1) * top / 2
    fit = np.polynomial.chebyshev.Chebyshev.fit(nodes, function(np.sqrt(nodes)), degree, domain=[0, top])
    return [float(c) for c in fit.convert(kind=np.polynomial.Polynomial).coef]


COS = fit_even(np.cos, 6)
SIN = fit_even(lambda t: np.sin(t) / t, 5)


def horner(coefs, u, scale):
    total = jnp.float32(coefs[-1] * scale)
    for c in coefs[-2::-1]:
        total = total * u + jnp.float32(c * scale)
    return total


def cos_sin(turn, scale):
    u = turn * turn
    return horner(COS, u, scale), turn * horner(SIN, u, scale)


def sign_table(count):
    both = lax.broadcasted_iota(jnp.int32, (count, count), 0) & lax.broadcasted_iota(jnp.int32, (count, count), 1)
    shift = 1
    while shift < count.bit_length():
        shift *= 2
    while shift > 1:
        shift //= 2
        both = both ^ (both >> shift)
    return (1 - 2 * (both & 1)).astype(jnp.float32).astype(jnp.bfloat16)


def mix_lead(x):
    n = x.shape[0]
    half = 1
    while half < n:
        y = x.reshape((n // (2 * half), 2, half) + x.shape[1:])
        x = jnp.stack([y[:, 0] + y[:, 1], y[:, 0] - y[:, 1]], axis=1).reshape(x.shape)
        half *= 2
    return x


def dot(a, b):
    return jnp.dot(a, b, preferred_element_type=jnp.float32)


def halves(x):
    hi = x.astype(jnp.bfloat16)
    return hi, (x - hi.astype(jnp.float32)).astype(jnp.bfloat16)


def mix_rows_lanes(rows, lanes, x, y):
    hi, lo = halves(jnp.concatenate([x, y], axis=1))
    both = dot(rows, hi) + dot(rows, lo)
    width = x.shape[1]
    out = []
    for part in (both[:, :width], both[:, width:]):
        hi, lo = halves(part)
        out.append(dot(hi, lanes) + dot(lo, lanes))
    return out


def kernel(
    na, nb, scales, wave_hbm, level_hbm, angle_hbm, out_ref,
    wave, level, angle, rows_table, lanes_table, mixed, send0, got0, send1, got1, levels, cosine, sine,
    load_sem, own_sem, ssem, rsem, level_sem,
):
    n = na * nb
    cuts, _, _, step, lanes = send0.shape
    qa, qb = lax.axis_index("qa"), lax.axis_index("qb")
    me = qa * nb + qb
    group = 4

    def flips(q, count):
        found = [q]
        bit = 1
        while bit < count:
            change = bit - 2 * bit * lax.rem(q // bit, 2)
            found = found + [f + change for f in found]
            bit *= 2
        return found

    to_as, to_bs = flips(qa, na), flips(qb, nb)
    order = [(ka, kb) for ka in far_first(na) for kb in range(nb) if ka or kb]
    peers = [(to_as[ka], to_bs[kb], to_as[ka] * nb + to_bs[kb]) for ka, kb in order]

    load_wave = pltpu.make_async_copy(wave_hbm, wave, load_sem.at[0])
    load_level = pltpu.make_async_copy(level_hbm, level, load_sem.at[1])
    load_angle = pltpu.make_async_copy(angle_hbm, angle, load_sem.at[2])
    load_level.start()
    load_angle.start()
    load_wave.start()

    barrier = pltpu.get_barrier_semaphore()
    for to_a, to_b, _ in peers[::-1]:
        pl.semaphore_signal(barrier, inc=1, device_id=(to_a, to_b), device_id_type=MESH)

    load_level.wait()
    pl.semaphore_wait(barrier, n - 1)

    def exchange(source, target, own, sent, got):
        pltpu.make_async_copy(source.at[me], target.at[me], own).start()
        for to_a, to_b, to in peers:
            pltpu.make_async_remote_copy(
                src_ref=source.at[to], dst_ref=target.at[me], send_sem=sent, recv_sem=got,
                device_id=(to_a, to_b), device_id_type=MESH,
            ).start()

    def received(source, target, own, got):
        pltpu.make_async_copy(source.at[me], target.at[me], own).wait()
        rest = target.at[pl.ds(0, n - 1)]
        pltpu.make_async_copy(rest, rest, got).wait()

    def left(source, sent):
        rest = source.at[pl.ds(0, n - 1)]
        pltpu.make_async_copy(rest, rest, sent).wait()

    exchange(level, levels, level_sem.at[0], level_sem.at[1], level_sem.at[2])
    rows_table[...] = sign_table(n * step)
    lanes_table[...] = sign_table(lanes)
    load_angle.wait()
    load_wave.wait()

    first = angle[0:1, :]

    @pl.loop(0, cuts)
    def _(cut):
        held = pl.ds(pl.multiple_of(cut * step, step), step)
        c, s = cos_sin(first * level[:, held, :].reshape(n * step, lanes), scales[0])
        x = wave[0, :, held, :].reshape(n * step, lanes)
        y = wave[1, :, held, :].reshape(n * step, lanes)
        done = mix_rows_lanes(rows_table[...], lanes_table[...], x * c + y * s, y * c - x * s)
        for part in range(2):
            mixed[cut, part] = done[part].reshape(n, step, lanes)

    for part in range(2):

        @pl.loop(0, n // group)
        def _(i):
            ds = pl.ds(i * group, group)
            send0[:, ds, part] = mix_lead(mixed[:, part, ds])

    @pl.loop(0, cuts)
    def _(cut):
        exchange(send0.at[cut], got0.at[cut], own_sem.at[0, cut], ssem.at[0, cut], rsem.at[0, cut])

    received(level, levels, level_sem.at[0], level_sem.at[2])
    second = angle[1:2, :]

    @pl.loop(0, n)
    def _(d):
        c, s = cos_sin(second * levels[d], scales[1])
        cosine[d] = c
        sine[d] = s

    @pl.loop(0, cuts)
    def _(cut):
        received(send0.at[cut], got0.at[cut], own_sem.at[0, cut], rsem.at[0, cut])
        held = pl.ds(pl.multiple_of(cut * step, step), step)
        x, y = mix_lead(got0[cut, :, 0]), mix_lead(got0[cut, :, 1])
        c, s = cosine[:, held, :], sine[:, held, :]
        send1[cut, :, 0] = mix_lead(x * c + y * s)
        send1[cut, :, 1] = mix_lead(y * c - x * s)
        exchange(send1.at[cut], got1.at[cut], own_sem.at[1, cut], ssem.at[1, cut], rsem.at[1, cut])

    @pl.loop(0, cuts)
    def _(cut):
        received(send1.at[cut], got1.at[cut], own_sem.at[1, cut], rsem.at[1, cut])
        x, y = (got1[cut, :, part].reshape(n * step, lanes) for part in range(2))
        done = mix_rows_lanes(rows_table[...], lanes_table[...], x, y)
        for part in range(2):
            mixed[cut, part] = done[part].reshape(n, step, lanes)

    for part in range(2):

        @pl.loop(0, n // group)
        def _(i):
            ds = pl.ds(i * group, group)
            done = mix_lead(mixed[:, part, ds])
            for cut in range(cuts):
                out_ref[part, ds, cut * step : (cut + 1) * step, :] = done[cut]

    left(level, level_sem.at[1])

    @pl.loop(0, cuts)
    def _(cut):
        left(send0.at[cut], ssem.at[0, cut])
        left(send1.at[cut], ssem.at[1, cut])


def far_first(count):
    quarter = count // 4
    low = [*range(0, quarter, 2), *range(1, quarter, 2)]
    return [high * quarter + k for high in (2, 3, 1, 0) for k in low] if quarter else range(count - 1, -1, -1)


STEP = 8


def body(wave_parts, level_table, phase_angles):
    na, nb = lax.axis_size("qa"), lax.axis_size("qb")
    n = na * nb
    _, blocks, rows, lanes = wave_parts.shape
    piece = blocks * rows // n
    step = min(STEP, piece)
    cuts = piece // step
    bits = (n * blocks * rows * lanes).bit_length() - 1
    scales = (2.0 ** -(bits // 2), 2.0 ** -(bits - bits // 2))
    hbm = pl.BlockSpec(memory_space=pl.ANY)
    f32 = jnp.float32
    flat = (2, n, piece, lanes)
    state = pltpu.VMEM((cuts, n, 2, step, lanes), f32)
    table = pltpu.VMEM((n, piece, lanes), f32)
    result = pl.pallas_call(
        functools.partial(kernel, na, nb, scales),
        out_shape=jax.ShapeDtypeStruct(flat, f32),
        in_specs=[hbm, hbm, hbm],
        out_specs=pl.BlockSpec(memory_space=pltpu.VMEM),
        scratch_shapes=[
            pltpu.VMEM(flat, f32),
            table,
            pltpu.VMEM(phase_angles.shape, f32),
            pltpu.VMEM((n * step, n * step), jnp.bfloat16),
            pltpu.VMEM((lanes, lanes), jnp.bfloat16),
            pltpu.VMEM((cuts, 2, n, step, lanes), f32),
            state, state, state, state, table, table, table,
            pltpu.SemaphoreType.DMA((3,)),
            pltpu.SemaphoreType.DMA((2, cuts)),
            pltpu.SemaphoreType.DMA((2, cuts)),
            pltpu.SemaphoreType.DMA((2, cuts)),
            pltpu.SemaphoreType.DMA((3,)),
        ],
        compiler_params=pltpu.CompilerParams(
            collective_id=0, has_side_effects=True, vmem_limit_bytes=62 * 2**20
        ),
    )(wave_parts.reshape(flat), level_table.reshape(n, piece, lanes), phase_angles)
    return result.reshape(wave_parts.shape)


def solution(mesh):
    in_specs = (P(None, ("qa", "qb"), None, None), P(("qa", "qb"), None, None), P())
    out_specs = P(None, ("qa", "qb"), None, None)
    return jax.shard_map(body, mesh=mesh, in_specs=in_specs, out_specs=out_specs, check_vma=False)
```

```python
import functools

import jax
import jax.numpy as jnp
import numpy as np
from jax import lax
from jax.experimental import pallas as pl
from jax.experimental.pallas import tpu as pltpu
from jax.sharding import PartitionSpec as P

MESH = pl.DeviceIdType.MESH
TURN_MOST = 2.5


def fit_even(function, degree):
    top = TURN_MOST**2
    nodes = (np.cos(np.pi * (np.arange(64) + 0.5) / 64) + 1) * top / 2
    fit = np.polynomial.chebyshev.Chebyshev.fit(nodes, function(np.sqrt(nodes)), degree, domain=[0, top])
    return [float(c) for c in fit.convert(kind=np.polynomial.Polynomial).coef]


COS = fit_even(np.cos, 6)
SIN = fit_even(lambda t: np.sin(t) / t, 5)


def horner(coefs, u, scale):
    total = jnp.float32(coefs[-1] * scale)
    for c in coefs[-2::-1]:
        total = total * u + jnp.float32(c * scale)
    return total


def cos_sin(turn, scale):
    u = turn * turn
    return horner(COS, u, scale), turn * horner(SIN, u, scale)


def sign_table(count):
    both = lax.broadcasted_iota(jnp.int32, (count, count), 0) & lax.broadcasted_iota(jnp.int32, (count, count), 1)
    shift = 1
    while shift < count.bit_length():
        shift *= 2
    while shift > 1:
        shift //= 2
        both = both ^ (both >> shift)
    return (1 - 2 * (both & 1)).astype(jnp.float32).astype(jnp.bfloat16)


def mix_lead(x):
    n = x.shape[0]
    half = 1
    while half < n:
        y = x.reshape((n // (2 * half), 2, half) + x.shape[1:])
        x = jnp.stack([y[:, 0] + y[:, 1], y[:, 0] - y[:, 1]], axis=1).reshape(x.shape)
        half *= 2
    return x


def dot(a, b):
    return jnp.dot(a, b, preferred_element_type=jnp.float32)


def halves(x):
    hi = x.astype(jnp.bfloat16)
    return hi, (x - hi.astype(jnp.float32)).astype(jnp.bfloat16)


def mix_rows_lanes(rows, lanes, x, y):
    hi, lo = halves(jnp.concatenate([x, y], axis=1))
    both = dot(rows, hi) + dot(rows, lo)
    width = x.shape[1]
    out = []
    for part in (both[:, :width], both[:, width:]):
        hi, lo = halves(part)
        out.append(dot(hi, lanes) + dot(lo, lanes))
    return out


def kernel(
    na, nb, scales, wave_hbm, level_hbm, angle_hbm, out_ref,
    wave, level, angle, rows_table, lanes_table, mixed, send0, got0, send1, got1, levels, cosine, sine,
    load_sem, own_sem, ssem, rsem, level_sem,
):
    n = na * nb
    cuts, _, _, step, lanes = send0.shape
    qa, qb = lax.axis_index("qa"), lax.axis_index("qb")
    me = qa * nb + qb
    group = 4

    def flips(q, count):
        found = [q]
        bit = 1
        while bit < count:
            change = bit - 2 * bit * lax.rem(q // bit, 2)
            found = found + [f + change for f in found]
            bit *= 2
        return found

    to_as, to_bs = flips(qa, na), flips(qb, nb)
    order = [(ka, kb) for ka in far_first(na) for kb in range(nb) if ka or kb]
    peers = [(to_as[ka], to_bs[kb], to_as[ka] * nb + to_bs[kb]) for ka, kb in order]

    load_wave = pltpu.make_async_copy(wave_hbm, wave, load_sem.at[0])
    load_level = pltpu.make_async_copy(level_hbm, level, load_sem.at[1])
    load_angle = pltpu.make_async_copy(angle_hbm, angle, load_sem.at[2])
    load_level.start()
    load_angle.start()
    load_wave.start()

    barrier = pltpu.get_barrier_semaphore()
    for to_a, to_b, _ in peers[::-1]:
        pl.semaphore_signal(barrier, inc=1, device_id=(to_a, to_b), device_id_type=MESH)

    load_level.wait()
    pl.semaphore_wait(barrier, n - 1)

    def exchange(source, target, own, sent, got):
        pltpu.make_async_copy(source.at[me], target.at[me], own).start()
        for to_a, to_b, to in peers:
            pltpu.make_async_remote_copy(
                src_ref=source.at[to], dst_ref=target.at[me], send_sem=sent, recv_sem=got,
                device_id=(to_a, to_b), device_id_type=MESH,
            ).start()

    def received(source, target, own, got):
        pltpu.make_async_copy(source.at[me], target.at[me], own).wait()
        rest = target.at[pl.ds(0, n - 1)]
        pltpu.make_async_copy(rest, rest, got).wait()

    def left(source, sent):
        rest = source.at[pl.ds(0, n - 1)]
        pltpu.make_async_copy(rest, rest, sent).wait()

    exchange(level, levels, level_sem.at[0], level_sem.at[1], level_sem.at[2])
    rows_table[...] = sign_table(n * step)
    lanes_table[...] = sign_table(lanes)
    load_angle.wait()
    load_wave.wait()

    first = angle[0:1, :]

    @pl.loop(0, cuts)
    def _(cut):
        held = pl.ds(pl.multiple_of(cut * step, step), step)
        c, s = cos_sin(first * level[:, held, :].reshape(n * step, lanes), scales[0])
        x = wave[0, :, held, :].reshape(n * step, lanes)
        y = wave[1, :, held, :].reshape(n * step, lanes)
        done = mix_rows_lanes(rows_table[...], lanes_table[...], x * c + y * s, y * c - x * s)
        for part in range(2):
            mixed[cut, part] = done[part].reshape(n, step, lanes)

    for part in range(2):

        @pl.loop(0, n // group)
        def _(i):
            ds = pl.ds(i * group, group)
            send0[:, ds, part] = mix_lead(mixed[:, part, ds])

    @pl.loop(0, cuts)
    def _(cut):
        exchange(send0.at[cut], got0.at[cut], own_sem.at[0, cut], ssem.at[0, cut], rsem.at[0, cut])

    received(level, levels, level_sem.at[0], level_sem.at[2])
    second = angle[1:2, :]

    @pl.loop(0, n)
    def _(d):
        c, s = cos_sin(second * levels[d], scales[1])
        cosine[d] = c
        sine[d] = s

    @pl.loop(0, cuts)
    def _(cut):
        received(send0.at[cut], got0.at[cut], own_sem.at[0, cut], rsem.at[0, cut])
        held = pl.ds(pl.multiple_of(cut * step, step), step)
        x, y = mix_lead(got0[cut, :, 0]), mix_lead(got0[cut, :, 1])
        c, s = cosine[:, held, :], sine[:, held, :]
        send1[cut, :, 0] = mix_lead(x * c + y * s)
        send1[cut, :, 1] = mix_lead(y * c - x * s)
        exchange(send1.at[cut], got1.at[cut], own_sem.at[1, cut], ssem.at[1, cut], rsem.at[1, cut])

    @pl.loop(0, cuts)
    def _(cut):
        received(send1.at[cut], got1.at[cut], own_sem.at[1, cut], rsem.at[1, cut])
        x, y = (got1[cut, :, part].reshape(n * step, lanes) for part in range(2))
        done = mix_rows_lanes(rows_table[...], lanes_table[...], x, y)
        for part in range(2):
            mixed[cut, part] = done[part].reshape(n, step, lanes)

    for part in range(2):

        @pl.loop(0, n // group)
        def _(i):
            ds = pl.ds(i * group, group)
            done = mix_lead(mixed[:, part, ds])
            for cut in range(cuts):
                out_ref[part, ds, cut * step : (cut + 1) * step, :] = done[cut]

    left(level, level_sem.at[1])

    @pl.loop(0, cuts)
    def _(cut):
        left(send0.at[cut], ssem.at[0, cut])
        left(send1.at[cut], ssem.at[1, cut])


def far_first(count):
    quarter = count // 4
    low = [*range(0, quarter, 2), *range(1, quarter, 2)]
    return [high * quarter + k for high in (2, 3, 1, 0) for k in low] if quarter else range(count - 1, -1, -1)


STEP = 16


def body(wave_parts, level_table, phase_angles):
    na, nb = lax.axis_size("qa"), lax.axis_size("qb")
    n = na * nb
    _, blocks, rows, lanes = wave_parts.shape
    piece = blocks * rows // n
    step = min(STEP, piece)
    cuts = piece // step
    bits = (n * blocks * rows * lanes).bit_length() - 1
    scales = (2.0 ** -(bits // 2), 2.0 ** -(bits - bits // 2))
    hbm = pl.BlockSpec(memory_space=pl.ANY)
    f32 = jnp.float32
    flat = (2, n, piece, lanes)
    state = pltpu.VMEM((cuts, n, 2, step, lanes), f32)
    table = pltpu.VMEM((n, piece, lanes), f32)
    result = pl.pallas_call(
        functools.partial(kernel, na, nb, scales),
        out_shape=jax.ShapeDtypeStruct(flat, f32),
        in_specs=[hbm, hbm, hbm],
        out_specs=pl.BlockSpec(memory_space=pltpu.VMEM),
        scratch_shapes=[
            pltpu.VMEM(flat, f32),
            table,
            pltpu.VMEM(phase_angles.shape, f32),
            pltpu.VMEM((n * step, n * step), jnp.bfloat16),
            pltpu.VMEM((lanes, lanes), jnp.bfloat16),
            pltpu.VMEM((cuts, 2, n, step, lanes), f32),
            state, state, state, state, table, table, table,
            pltpu.SemaphoreType.DMA((3,)),
            pltpu.SemaphoreType.DMA((2, cuts)),
            pltpu.SemaphoreType.DMA((2, cuts)),
            pltpu.SemaphoreType.DMA((2, cuts)),
            pltpu.SemaphoreType.DMA((3,)),
        ],
        compiler_params=pltpu.CompilerParams(
            collective_id=0, has_side_effects=True, vmem_limit_bytes=62 * 2**20
        ),
    )(wave_parts.reshape(flat), level_table.reshape(n, piece, lanes), phase_angles)
    return result.reshape(wave_parts.shape)


def solution(mesh):
    in_specs = (P(None, ("qa", "qb"), None, None), P(("qa", "qb"), None, None), P())
    out_specs = P(None, ("qa", "qb"), None, None)
    return jax.shard_map(body, mesh=mesh, in_specs=in_specs, out_specs=out_specs, check_vma=False)
```
